32 devices in a mesh: groups: 2 (over y), frame: 4 (over z), space: 2 (over x), head: 2 (over core).
Axes of the slice: x: 2, y: 2, z: 4, core: 2. Of those that a mesh axis runs over, the one named last changes fastest.
Arguments:
- queries: bfloat16 [8, 512, 3072], P(('groups', 'frame'), 'space', 'head'), parts along dimension 0, may hold values from -6 to 6
- key_states: bfloat16 [8, 512, 3072], P(('groups', 'frame'), 'space', 'head'), parts along dimension 0, may hold values from -24 to 24
- value_states: bfloat16 [8, 512, 3072], P(('groups', 'frame'), 'space', 'head'), parts along dimension 0, may hold values from -6 to 6
- profile: int32 [24], replicated, may hold values from 0 to 1, as said below
- window: int32 [24], replicated, may hold values from 1 to 4, as said below
Outputs:
- attended: bfloat16 [8, 512, 3072], P(('groups', 'frame'), 'space', 'head'), parts along dimension 0
The draws below stay inside these ranges and needn't reach their ends.
There are 2 independent parts, one for each index of `groups`. The reference program is written for one: setup_inputs(seed, part) draws one part's arguments, and reference() takes and returns one part's arrays. A program takes and returns all parts, laid end to end along the dimension named above; an argument that names none is the same for every part. Nothing has to cross between parts.
Inputs may be any that keep to these rules, and one draw needn't show every extreme that they name: `profile`: 1 marks a head of frame-local attention, 0 a head of attention over a window of frames; exactly half of the 24 heads are marked 1. Some head marked 0 in profile has window 4.
All inputs are finite; a program needn't handle non-finite values.
Results may differ from the reference program's by a relative error of at most 0.0055.
Values may be sent and summed in bfloat16 or wider, within the bound.
A program may use at most 64 MiB of HBM per device.

```python
import jax
import jax.numpy as jnp
from jax import lax

H = 24
HD = 128
WMAX = 4
NTOK = 512
FRAMES = 4


def drawn_pair(key):
    base = jax.random.fold_in(key, 7)
    key_query, key_keys = jax.random.split(base, 2)
    shape_full = (FRAMES, NTOK, H * HD)
    query_draw = jnp.clip(jax.random.normal(key_query, shape_full, jnp.float32), -6.0, 6.0)
    key_draw = jnp.clip(jax.random.normal(key_keys, shape_full, jnp.float32), -6.0, 6.0)
    return (query_draw, key_draw)


def draw_queries(key, part):
    return drawn_pair(key)[0].astype(jnp.bfloat16)


def draw_key_states(key, part):
    return drawn_pair(key)[1].astype(jnp.bfloat16)


def head_classes(key):
    order = jax.random.permutation(jax.random.fold_in(key, 11), H)
    return (order < H // 2).astype(jnp.int32)


def draw_profile(key, part):
    return head_classes(key)


def draw_window(key, part):
    classes = head_classes(key)
    reaches = jax.random.randint(jax.random.fold_in(key, 13), (H,), 1, WMAX + 1)
    first_window = jnp.argmin(classes)
    return reaches.at[first_window].set(WMAX).astype(jnp.int32)


def level_of(rng, dims, cuts, low, high):
    def one(dim, parts):
        heights = jax.random.uniform(jax.random.fold_in(jax.random.fold_in(rng, 6), dim), (parts,), jnp.float32, low / len(cuts), high / len(cuts))
        return jnp.repeat(jnp.exp(heights), dims[dim] // parts).reshape((-1,) + (1,) * (len(dims) - dim - 1))

    loudness = one(*cuts[0])
    for cut in cuts[1:]:
        loudness = loudness * one(*cut)
    return loudness


def normal_values(key, shape, spread, bound, pieces=(), kind=jnp.bfloat16):
    drawn = jax.random.normal(key, shape, jnp.float32) * spread
    if len(pieces) > 0:
        drawn = level_of(key, shape, pieces, -0.22, 0.18) * drawn
    return jnp.clip(drawn, min=-bound, max=bound).astype(kind)


def setup_inputs(seed: int = 0, part: int = 0) -> dict:
    streams_of = jax.random.split(jax.random.key(seed), 6)
    part_splits = jax.random.split(jax.random.fold_in(streams_of[5], part), 6)
    return {
        "queries": draw_queries(jax.random.fold_in(jax.random.fold_in(streams_of[5], part), 71), part),
        "key_states": draw_key_states(jax.random.fold_in(jax.random.fold_in(streams_of[5], part), 71), part),
        "value_states": normal_values(part_splits[2], (FRAMES, NTOK, H * HD), 1.0, 6.0, ((0, 4), (1, 2), (2, 2))),
        "profile": draw_profile(jax.random.fold_in(streams_of[5], 71), part),
        "window": draw_window(jax.random.fold_in(streams_of[5], 71), part),
    }


def spatial_frames(queries, key_states, value_states):
    token_count = queries.shape[1]
    scale = HD ** -0.5

    def one_frame(item):
        query_frame, key_frame, value_frame = item
        query_heads = jnp.moveaxis(query_frame.reshape(token_count, H, HD), 1, 0)
        key_heads = jnp.moveaxis(key_frame.reshape(token_count, H, HD), 1, 0)
        value_heads = jnp.moveaxis(value_frame.reshape(token_count, H, HD), 1, 0)

        def one_head(triple):
            query_one, key_one, value_one = triple
            scores = jnp.dot(query_one, key_one.T, preferred_element_type=jnp.float32) * scale
            peak = jnp.max(scores, axis=1, keepdims=True)
            weights = jnp.exp(scores - peak)
            denominator = jnp.sum(weights, axis=1, keepdims=True)
            numerator = jnp.dot(weights.astype(jnp.bfloat16), value_one, preferred_element_type=jnp.float32)
            return numerator / denominator

        result = lax.map(one_head, (query_heads, key_heads, value_heads))
        return jnp.moveaxis(result, 0, 1)

    return lax.map(one_frame, (queries, key_states, value_states))


def temporal_frames(queries, key_states, value_states, window):
    frame_count, token_count = queries.shape[0], queries.shape[1]
    scale = HD ** -0.5
    shape_four = (frame_count, token_count, H, HD)
    query_heads = queries.reshape(shape_four).astype(jnp.float32)
    padding = ((WMAX, WMAX), (0, 0), (0, 0), (0, 0))
    key_padded = jnp.pad(key_states.reshape(shape_four), padding)
    value_padded = jnp.pad(value_states.reshape(shape_four), padding)
    frame_ids = jnp.arange(frame_count, dtype=jnp.int32)
    score_list = []
    for offset in range(-WMAX, WMAX + 1):
        near_keys = key_padded[WMAX + offset:WMAX + offset + frame_count]
        raw_scores = jnp.einsum("fnhd,fnhd->fnh", query_heads, near_keys.astype(jnp.float32)) * scale
        in_range = (frame_ids + offset >= 0) & (frame_ids + offset < frame_count)
        inside = in_range[:, None, None] & (window >= abs(offset))[None, None, :]
        score_list.append(jnp.where(inside, raw_scores, -1e30))
    scores = jnp.stack(score_list)
    peak = jnp.max(scores, axis=0)
    weights = jnp.exp(scores - peak[None])
    denominator = jnp.sum(weights, axis=0)
    rounded = weights.astype(jnp.bfloat16).astype(jnp.float32)
    numerator = jnp.zeros(shape_four, jnp.float32)
    for index, offset in enumerate(range(-WMAX, WMAX + 1)):
        near_values = value_padded[WMAX + offset:WMAX + offset + frame_count].astype(jnp.float32)
        numerator = numerator + rounded[index][..., None] * near_values
    return numerator / denominator[..., None]


def reference(queries, key_states, value_states, profile, window):
    spatial_part = spatial_frames(queries, key_states, value_states)
    temporal_part = temporal_frames(queries, key_states, value_states, window)
    chosen = jnp.where((profile == 1)[None, None, :, None], spatial_part, temporal_part)
    return chosen.reshape(queries.shape).astype(jnp.bfloat16)
```

```python
import functools

import jax
import jax.numpy as jnp
from jax import lax
from jax.experimental import pallas as pl
from jax.experimental.pallas import tpu as pltpu
from jax.sharding import PartitionSpec as P

HD = 128
WMAX = 4
MESH = pl.DeviceIdType.MESH


def kernel(
    frames, spaces, cores, prof_ref, win_ref, q_ref, k_ref, v_ref, out_ref,
    full_q, full_k, full_v, kv, tsend, trecv, tout, res, pos, tab,
    loc_sem, d_send, d_recv, s_send, s_recv, t_send, t_recv, o_send, o_recv, r_send, r_recv,
):
    rows = q_ref.shape[1]
    here = q_ref.shape[2] // HD
    heads = here * cores
    share = here // 2
    part = rows // frames
    scale = HD ** (-0.5)
    f = lax.axis_index("frame")
    x = lax.axis_index("space")
    c = lax.axis_index("head")
    others_f = [lax.rem(f + d, frames) for d in range(1, frames)]
    others_x = [lax.rem(x + d, spaces) for d in range(1, spaces)]
    others_c = [lax.rem(c + d, cores) for d in range(1, cores)]
    side = f // (frames // 2)
    far_first = [
        lax.rem(f + (1 - side) * (frames - 1 - i) + side * (1 + i), frames)
        for i in range(frames - 1)
    ]

    def remote(src, dst, send, recv, **target):
        return pltpu.make_async_remote_copy(
            src_ref=src, dst_ref=dst, send_sem=send, recv_sem=recv,
            device_id=target, device_id_type=MESH,
        )

    pairs = ((k_ref, full_k), (v_ref, full_v), (q_ref, full_q))

    def lanes(h):
        return pl.ds(pl.multiple_of(h * HD, HD), HD)

    def own(full):
        return full.at[pl.ds(c * here, here)]

    for n, (src, full) in enumerate(pairs):
        def local_start(h, _):
            pltpu.make_async_copy(
                src.at[0, :, lanes(h)], full.at[c * here + h], loc_sem.at[n]
            ).start()
            return 0

        lax.fori_loop(0, here, local_start, 0)

    barrier = pltpu.get_barrier_semaphore()
    for other in others_c:
        pl.semaphore_signal(barrier, inc=1, device_id={"head": other}, device_id_type=MESH)
    for other in others_x:
        pl.semaphore_signal(barrier, inc=1, device_id={"space": other}, device_id_type=MESH)
    for other in others_f:
        pl.semaphore_signal(barrier, inc=1, device_id={"frame": other}, device_id_type=MESH)
    pl.semaphore_wait(barrier, len(others_c) + len(others_x) + len(others_f))

    for n, (src, full) in enumerate(pairs):
        for other in others_c:
            def core_start(h, _):
                remote(
                    src.at[0, :, lanes(h)], full.at[c * here + h],
                    d_send.at[other, n], d_recv.at[c, n], head=other,
                ).start()
                return 0

            lax.fori_loop(0, here, core_start, 0)

    in_space = jnp.int32(0)
    in_window = jnp.int32(0)
    for h in range(heads):
        p = prof_ref[h]
        rank = p * in_space + (1 - p) * in_window
        core = sum((rank >= share * e).astype(jnp.int32) for e in range(1, cores))
        place = rank + core * (here - share) + (1 - p) * share
        pos[h] = jnp.clip(place, 0, heads - 1)
        in_space = in_space + p
        in_window = in_window + (1 - p)

    def fill(slot, _):
        first = c * here + slot
        second = first + share
        id_s = jnp.int32(0)
        id_w = jnp.int32(0)
        reach = jnp.int32(0)
        for h in range(heads):
            id_s = id_s + jnp.where(pos[h] == first, h, 0)
            is_w = pos[h] == second
            id_w = id_w + jnp.where(is_w, h, 0)
            reach = reach + jnp.where(is_w, win_ref[h], 0)
        tab[0, slot] = jnp.clip(id_s, 0, heads - 1)
        tab[1, slot] = jnp.clip(id_w, 0, heads - 1)
        tab[2, slot] = reach
        return 0

    lax.fori_loop(0, share, fill, 0)

    for n, (src, full) in enumerate(pairs):
        for other in others_c:
            theirs = full.at[pl.ds(other * here, here)]
            remote(theirs, theirs, d_send.at[other, n], d_recv.at[other, n], head=other).wait_recv()
        pltpu.make_async_copy(own(full), own(full), loc_sem.at[n]).wait()

    def pick(full, head):
        return full[head]

    def window_copy(j, other):
        return remote(
            tsend.at[j, other], trecv.at[f, j], t_send.at[other, j], t_recv.at[f, j], frame=other
        )

    def window_gather(j, _):
        head = tab[1, j]
        for n, full in enumerate((full_q, full_k, full_v)):
            block = pick(full, head)
            for g in range(frames):
                tsend[j, g, n] = block[g * part:(g + 1) * part]

        @pl.when(j > 0)
        def _():
            for other in far_first:
                window_copy(j - 1, other).start()

        return 0

    lax.fori_loop(0, share, window_gather, 0)

    my_rows = pl.ds(pl.multiple_of(x * rows, rows), rows)

    def space_copy(j, other):
        return remote(
            kv.at[j, :, my_rows], kv.at[j, :, my_rows], s_send.at[other, j], s_recv.at[x, j], space=other
        )

    def space_gather(j, _):
        head = tab[0, j]
        kv[j, 0, my_rows] = pick(full_k, head)
        kv[j, 1, my_rows] = pick(full_v, head)

        @pl.when(j == 0)
        def _():
            for other in far_first:
                window_copy(share - 1, other).start()

        @pl.when(j > 0)
        def _():
            for other in others_x:
                space_copy(j - 1, other).start()

        return 0

    lax.fori_loop(0, share, space_gather, 0)
    mine = pl.ds(pl.multiple_of(f * part, part), part)

    def out_copy(j, other):
        return remote(
            tout.at[j, other], res.at[c * here + share + j, mine], o_send.at[other, j], o_recv.at[f, j], frame=other
        )

    def back_copy(slot, other):
        return remote(
            res.at[c * here + slot], res.at[c * here + slot], r_send.at[other, slot], r_recv.at[c, slot], head=other
        )

    for other in others_x:
        space_copy(share - 1, other).start()

    def step(j, _):
        for other in others_f:
            remote(
                tsend.at[j, other], trecv.at[other, j], t_send.at[other, j], t_recv.at[other, j], frame=other
            ).wait_recv()
        trecv[f, j] = tsend[j, f]
        reach = tab[2, j]
        qs = [trecv[g, j, 0].astype(jnp.float32) for g in range(frames)]
        ks = [trecv[g, j, 1].astype(jnp.float32) for g in range(frames)]
        vs = [trecv[g, j, 2].astype(jnp.float32) for g in range(frames)]
        for g in range(frames):
            near = [m for m in range(frames) if abs(m - g) <= WMAX]
            scores = []
            for m in near:
                raw = jnp.sum(qs[g] * ks[m], axis=-1, keepdims=True) * scale
                scores.append(jnp.where(reach >= abs(m - g), raw, -1e30))
            peak = functools.reduce(jnp.maximum, scores)
            weights = [jnp.exp(s - peak) for s in scores]
            total = functools.reduce(jnp.add, weights)
            acc = functools.reduce(
                jnp.add,
                [w.astype(jnp.bfloat16).astype(jnp.float32) * vs[m] for w, m in zip(weights, near)],
            )
            tout[j, g] = (acc / total).astype(jnp.bfloat16)
        res[c * here + share + j, mine] = tout[j, f]

        for other in others_x:
            other_rows = pl.ds(pl.multiple_of(other * rows, rows), rows)
            remote(
                kv.at[j, :, other_rows], kv.at[j, :, other_rows],
                s_send.at[other, j], s_recv.at[other, j], space=other,
            ).wait_recv()
        query = pick(full_q, tab[0, j])
        scores = lax.dot_general(
            query, kv[j, 0], (((1,), (1,)), ((), ())), preferred_element_type=jnp.float32
        ) * scale
        peak = jnp.max(scores, axis=1, keepdims=True)
        weights = jnp.exp(scores - peak)
        total = jnp.sum(weights, axis=1, keepdims=True)
        acc = jnp.dot(weights.astype(jnp.bfloat16), kv[j, 1], preferred_element_type=jnp.float32)
        res[c * here + j] = (acc / total).astype(jnp.bfloat16)

        for other in far_first:
            out_copy(j, other).start()

        @pl.when(j > 0)
        def _():
            for other in others_c:
                back_copy(j - 1, other).start()

        return 0

    lax.fori_loop(0, share, step, 0)
    for other in others_c:
        back_copy(share - 1, other).start()

    def forward(j, _):
        for other in others_f:
            theirs = pl.ds(pl.multiple_of(other * part, part), part)
            remote(
                tout.at[j, other], res.at[c * here + share + j, theirs], o_send.at[other, j], o_recv.at[other, j],
                frame=other,
            ).wait_recv()
        for other in others_c:
            back_copy(share + j, other).start()
        return 0

    lax.fori_loop(0, share, forward, 0)

    def arrive(slot, _):
        for other in others_c:
            remote(
                res.at[c * here + slot], res.at[other * here + slot], r_send.at[other, slot], r_recv.at[other, slot], head=other
            ).wait_recv()
        return 0

    lax.fori_loop(0, 2 * share, arrive, 0)

    for i in range(here):
        where = pos[c * here + i]
        out_ref[0, :, i * HD:(i + 1) * HD] = res[where]

    for n, (src, full) in enumerate(pairs):
        for other in others_c:
            remote(own(full), own(full), d_send.at[other, n], d_recv.at[c, n], head=other).wait_send()

    def drain(j, _):
        for other in others_f:
            window_copy(j, other).wait_send()
            out_copy(j, other).wait_send()
        for other in others_x:
            space_copy(j, other).wait_send()
        for other in others_c:
            back_copy(j, other).wait_send()
            back_copy(share + j, other).wait_send()
        return 0

    lax.fori_loop(0, share, drain, 0)


def local(sizes, queries, key_states, value_states, profile, window):
    frames, spaces, cores = sizes
    rows = queries.shape[1]
    here = queries.shape[2] // HD
    share = here // 2
    part = rows // frames
    any_space = pl.BlockSpec(memory_space=pl.ANY)
    smem = pl.BlockSpec(memory_space=pltpu.SMEM)
    bf = jnp.bfloat16
    dma = pltpu.SemaphoreType.DMA
    return pl.pallas_call(
        functools.partial(kernel, frames, spaces, cores),
        out_shape=jax.ShapeDtypeStruct(queries.shape, queries.dtype),
        in_specs=[smem, smem, any_space, any_space, any_space],
        out_specs=pl.BlockSpec(memory_space=pltpu.VMEM),
        scratch_shapes=[
            pltpu.VMEM((cores * here, rows, HD), bf),
            pltpu.VMEM((cores * here, rows, HD), bf),
            pltpu.VMEM((cores * here, rows, HD), bf),
            pltpu.VMEM((share, 2, spaces * rows, HD), bf),
            pltpu.VMEM((share, frames, 3, part, HD), bf),
            pltpu.VMEM((frames, share, 3, part, HD), bf),
            pltpu.VMEM((share, frames, part, HD), bf),
            pltpu.VMEM((cores * 2 * share, rows, HD), bf),
            pltpu.SMEM((here * cores,), jnp.int32),
            pltpu.SMEM((3, share), jnp.int32),
            dma((3,)),
            dma((cores, 3)),
            dma((cores, 3)),
            dma((spaces, share)),
            dma((spaces, share)),
            dma((frames, share)),
            dma((frames, share)),
            dma((frames, share)),
            dma((frames, share)),
            dma((cores, 2 * share)),
            dma((cores, 2 * share)),
        ],
        compiler_params=pltpu.CompilerParams(
            collective_id=0, has_side_effects=True, vmem_limit_bytes=60 * 1024 * 1024
        ),
    )(profile, window, queries, key_states, value_states)


def solution(mesh):
    spec = P(("groups", "frame"), "space", "head")
    sizes = (mesh.shape["frame"], mesh.shape["space"], mesh.shape["head"])
    return jax.shard_map(
        functools.partial(local, sizes),
        mesh=mesh,
        in_specs=(spec, spec, spec, P(), P()),
        out_specs=spec,
        check_vma=False,
    )
```

```python
import functools

import jax
import jax.numpy as jnp
from jax import lax
from jax.experimental import pallas as pl
from jax.experimental.pallas import tpu as pltpu
from jax.sharding import PartitionSpec as P

HD = 128
WMAX = 4
EARLY = 2
MESH = pl.DeviceIdType.MESH


def kernel(
    frames, spaces, cores, prof_ref, win_ref, q_ref, k_ref, v_ref, out_ref,
    full_q, full_k, full_v, kv, tsend, trecv, tout, res, pos, tab,
    loc_sem, d_send, d_recv, s_send, s_recv, t_send, t_recv, o_send, o_recv, r_send, r_recv,
):
    rows = q_ref.shape[1]
    here = q_ref.shape[2] // HD
    heads = here * cores
    share = here // 2
    part = rows // frames
    scale = HD ** (-0.5)
    f = lax.axis_index("frame")
    x = lax.axis_index("space")
    c = lax.axis_index("head")
    others_f = [lax.rem(f + d, frames) for d in range(1, frames)]
    others_x = [lax.rem(x + d, spaces) for d in range(1, spaces)]
    others_c = [lax.rem(c + d, cores) for d in range(1, cores)]
    side = f // (frames // 2)
    far_first = [
        lax.rem(f + (1 - side) * (frames - 1 - i) + side * (1 + i), frames)
        for i in range(frames - 1)
    ]

    def remote(src, dst, send, recv, **target):
        return pltpu.make_async_remote_copy(
            src_ref=src, dst_ref=dst, send_sem=send, recv_sem=recv,
            device_id=target, device_id_type=MESH,
        )

    pairs = ((k_ref, full_k), (v_ref, full_v), (q_ref, full_q))

    def lanes(h):
        return pl.ds(pl.multiple_of(h * HD, HD), HD)

    def own(full):
        return full.at[pl.ds(c * here, here)]

    for n, (src, full) in enumerate(pairs):
        def local_start(h, _):
            pltpu.make_async_copy(
                src.at[0, :, lanes(h)], full.at[c * here + h], loc_sem.at[n]
            ).start()
            return 0

        lax.fori_loop(0, here, local_start, 0)

    barrier = pltpu.get_barrier_semaphore()
    for other in others_c:
        pl.semaphore_signal(barrier, inc=1, device_id={"head": other}, device_id_type=MESH)
    for other in others_x:
        pl.semaphore_signal(barrier, inc=1, device_id={"space": other}, device_id_type=MESH)
    for other in others_f:
        pl.semaphore_signal(barrier, inc=1, device_id={"frame": other}, device_id_type=MESH)
    pl.semaphore_wait(barrier, len(others_c) + len(others_x) + len(others_f))

    for n, (src, full) in enumerate(pairs):
        for other in others_c:
            def core_start(h, _):
                remote(
                    src.at[0, :, lanes(h)], full.at[c * here + h],
                    d_send.at[other, n], d_recv.at[c, n], head=other,
                ).start()
                return 0

            lax.fori_loop(0, here, core_start, 0)

    in_space = jnp.int32(0)
    in_window = jnp.int32(0)
    for h in range(heads):
        p = prof_ref[h]
        rank = p * in_space + (1 - p) * in_window
        core = sum((rank >= share * e).astype(jnp.int32) for e in range(1, cores))
        place = rank + core * (here - share) + (1 - p) * share
        pos[h] = jnp.clip(place, 0, heads - 1)
        in_space = in_space + p
        in_window = in_window + (1 - p)

    def fill(slot, _):
        first = c * here + slot
        second = first + share
        id_s = jnp.int32(0)
        id_w = jnp.int32(0)
        reach = jnp.int32(0)
        for h in range(heads):
            id_s = id_s + jnp.where(pos[h] == first, h, 0)
            is_w = pos[h] == second
            id_w = id_w + jnp.where(is_w, h, 0)
            reach = reach + jnp.where(is_w, win_ref[h], 0)
        tab[0, slot] = jnp.clip(id_s, 0, heads - 1)
        tab[1, slot] = jnp.clip(id_w, 0, heads - 1)
        tab[2, slot] = reach
        return 0

    lax.fori_loop(0, share, fill, 0)

    my_rows = pl.ds(pl.multiple_of(x * rows, rows), rows)
    mine = pl.ds(pl.multiple_of(f * part, part), part)

    def pick(full, head):
        return full[head]

    def window_copy(j, other):
        return remote(
            tsend.at[j, other], trecv.at[f, j], t_send.at[other, j], t_recv.at[f, j], frame=other
        )

    def window_piece(j, n, other):
        return remote(
            tsend.at[j, other, n], trecv.at[f, j, n], t_send.at[other, j], t_recv.at[f, j], frame=other
        )

    def space_copy(j, other):
        return remote(
            kv.at[j, :, my_rows], kv.at[j, :, my_rows], s_send.at[other, j], s_recv.at[x, j], space=other
        )

    early = min(EARLY, share)
    for n, (src, full) in enumerate(pairs):
        for other in others_c:
            theirs = full.at[pl.ds(other * here, here)]
            remote(theirs, theirs, d_send.at[other, n], d_recv.at[other, n], head=other).wait_recv()
        pltpu.make_async_copy(own(full), own(full), loc_sem.at[n]).wait()

        def window_gather(j, _):
            block = pick(full, tab[1, j])
            for g in range(frames):
                tsend[j, g, n] = block[g * part:(g + 1) * part]
            return 0

        lax.fori_loop(0, share, window_gather, 0)

        def window_early(j, _):
            for other in far_first:
                window_piece(j, n, other).start()
            return 0

        lax.fori_loop(0, early, window_early, 0)

    def window_late(j, _):
        for other in far_first:
            window_copy(j, other).start()
        return 0

    lax.fori_loop(early, share, window_late, 0)

    def space_gather(j, _):
        head = tab[0, j]
        kv[j, 0, my_rows] = pick(full_k, head)
        kv[j, 1, my_rows] = pick(full_v, head)

        @pl.when(j > 0)
        def _():
            for other in others_x:
                space_copy(j - 1, other).start()

        return 0

    lax.fori_loop(0, share, space_gather, 0)

    def out_copy(j, other):
        return remote(
            tout.at[j, other], res.at[c * here + share + j, mine], o_send.at[other, j], o_recv.at[f, j], frame=other
        )

    def back_copy(slot, other):
        return remote(
            res.at[c * here + slot], res.at[c * here + slot], r_send.at[other, slot], r_recv.at[c, slot], head=other
        )

    for other in others_x:
        space_copy(share - 1, other).start()

    def step(j, _):
        for other in others_f:
            remote(
                tsend.at[j, other], trecv.at[other, j], t_send.at[other, j], t_recv.at[other, j], frame=other
            ).wait_recv()
        trecv[f, j] = tsend[j, f]
        reach = tab[2, j]
        qs = [trecv[g, j, 2].astype(jnp.float32) for g in range(frames)]
        ks = [trecv[g, j, 0].astype(jnp.float32) for g in range(frames)]
        vs = [trecv[g, j, 1].astype(jnp.float32) for g in range(frames)]
        for g in range(frames):
            near = [m for m in range(frames) if abs(m - g) <= WMAX]
            scores = []
            for m in near:
                raw = jnp.sum(qs[g] * ks[m], axis=-1, keepdims=True) * scale
                scores.append(jnp.where(reach >= abs(m - g), raw, -1e30))
            peak = functools.reduce(jnp.maximum, scores)
            weights = [jnp.exp(s - peak) for s in scores]
            total = functools.reduce(jnp.add, weights)
            acc = functools.reduce(
                jnp.add,
                [w.astype(jnp.bfloat16).astype(jnp.float32) * vs[m] for w, m in zip(weights, near)],
            )
            tout[j, g] = (acc / total).astype(jnp.bfloat16)
        res[c * here + share + j, mine] = tout[j, f]

        for other in others_x:
            other_rows = pl.ds(pl.multiple_of(other * rows, rows), rows)
            remote(
                kv.at[j, :, other_rows], kv.at[j, :, other_rows],
                s_send.at[other, j], s_recv.at[other, j], space=other,
            ).wait_recv()
        query = pick(full_q, tab[0, j])
        scores = lax.dot_general(
            query, kv[j, 0], (((1,), (1,)), ((), ())), preferred_element_type=jnp.float32
        ) * scale
        peak = jnp.max(scores, axis=1, keepdims=True)
        weights = jnp.exp(scores - peak)
        total = jnp.sum(weights, axis=1, keepdims=True)
        acc = jnp.dot(weights.astype(jnp.bfloat16), kv[j, 1], preferred_element_type=jnp.float32)
        res[c * here + j] = (acc / total).astype(jnp.bfloat16)

        for other in far_first:
            out_copy(j, other).start()

        @pl.when(j > 0)
        def _():
            for other in others_c:
                back_copy(j - 1, other).start()

        return 0

    lax.fori_loop(0, share, step, 0)
    for other in others_c:
        back_copy(share - 1, other).start()

    def forward(j, _):
        for other in others_f:
            theirs = pl.ds(pl.multiple_of(other * part, part), part)
            remote(
                tout.at[j, other], res.at[c * here + share + j, theirs], o_send.at[other, j], o_recv.at[other, j],
                frame=other,
            ).wait_recv()
        for other in others_c:
            back_copy(share + j, other).start()
        return 0

    lax.fori_loop(0, share, forward, 0)

    def arrive(slot, _):
        for other in others_c:
            remote(
                res.at[c * here + slot], res.at[other * here + slot], r_send.at[other, slot], r_recv.at[other, slot], head=other
            ).wait_recv()
        return 0

    lax.fori_loop(0, 2 * share, arrive, 0)

    for i in range(here):
        where = pos[c * here + i]
        out_ref[0, :, i * HD:(i + 1) * HD] = res[where]

    for n, (src, full) in enumerate(pairs):
        for other in others_c:
            remote(own(full), own(full), d_send.at[other, n], d_recv.at[c, n], head=other).wait_send()

    def drain(j, _):
        for other in others_f:
            window_copy(j, other).wait_send()
            out_copy(j, other).wait_send()
        for other in others_x:
            space_copy(j, other).wait_send()
        for other in others_c:
            back_copy(j, other).wait_send()
            back_copy(share + j, other).wait_send()
        return 0

    lax.fori_loop(0, share, drain, 0)


def local(sizes, queries, key_states, value_states, profile, window):
    frames, spaces, cores = sizes
    rows = queries.shape[1]
    here = queries.shape[2] // HD
    share = here // 2
    part = rows // frames
    any_space = pl.BlockSpec(memory_space=pl.ANY)
    smem = pl.BlockSpec(memory_space=pltpu.SMEM)
    bf = jnp.bfloat16
    dma = pltpu.SemaphoreType.DMA
    return pl.pallas_call(
        functools.partial(kernel, frames, spaces, cores),
        out_shape=pltpu.VMEM(queries.shape, queries.dtype),
        in_specs=[smem, smem, any_space, any_space, any_space],
        out_specs=pl.BlockSpec(memory_space=pltpu.VMEM),
        scratch_shapes=[
            pltpu.VMEM((cores * here, rows, HD), bf),
            pltpu.VMEM((cores * here, rows, HD), bf),
            pltpu.VMEM((cores * here, rows, HD), bf),
            pltpu.VMEM((share, 2, spaces * rows, HD), bf),
            pltpu.VMEM((share, frames, 3, part, HD), bf),
            pltpu.VMEM((frames, share, 3, part, HD), bf),
            pltpu.VMEM((share, frames, part, HD), bf),
            pltpu.VMEM((cores * 2 * share, rows, HD), bf),
            pltpu.SMEM((here * cores,), jnp.int32),
            pltpu.SMEM((3, share), jnp.int32),
            dma((3,)),
            dma((cores, 3)),
            dma((cores, 3)),
            dma((spaces, share)),
            dma((spaces, share)),
            dma((frames, share)),
            dma((frames, share)),
            dma((frames, share)),
            dma((frames, share)),
            dma((cores, 2 * share)),
            dma((cores, 2 * share)),
        ],
        compiler_params=pltpu.CompilerParams(
            collective_id=0, has_side_effects=True, vmem_limit_bytes=60 * 1024 * 1024
        ),
    )(profile, window, queries, key_states, value_states)


def solution(mesh):
    spec = P(("groups", "frame"), "space", "head")
    sizes = (mesh.shape["frame"], mesh.shape["space"], mesh.shape["head"])
    return jax.shard_map(
        functools.partial(local, sizes),
        mesh=mesh,
        in_specs=(spec, spec, spec, P(), P()),
        out_specs=spec,
        check_vma=False,
    )
```

```python
import functools

import jax
import jax.numpy as jnp
from jax import lax
from jax.experimental import pallas as pl
from jax.experimental.pallas import tpu as pltpu
from jax.sharding import PartitionSpec as P

HD = 128
WMAX = 4
MESH = pl.DeviceIdType.MESH


def kernel(
    frames, spaces, cores, prof_hbm, win_hbm, q_ref, k_ref, v_ref, out_ref,
    full, mine_first, theirs, squery, kv, tsend, trecv, tout, res,
    prof_ref, win_ref, pos, place, order, reaches, tab,
    loc_sem, d_send, d_recv, s_send, s_recv, t_send, t_recv, o_send, o_recv, r_send, r_recv,
):
    rows = q_ref.shape[1]
    here = q_ref.shape[2] // HD
    share = here // 2
    part = rows // frames
    scale = HD ** (-0.5)
    f = lax.axis_index("frame")
    x = lax.axis_index("space")
    c = lax.axis_index("head")
    others_f = [lax.rem(f + d, frames) for d in range(1, frames)]
    others_x = [lax.rem(x + d, spaces) for d in range(1, spaces)]
    others_c = [lax.rem(c + d, cores) for d in range(1, cores)]
    side = f // (frames // 2)
    far_first = [
        lax.rem(f + (1 - side) * (frames - 1 - i) + side * (1 + i), frames)
        for i in range(frames - 1)
    ]

    def remote(src, dst, send, recv, **target):
        return pltpu.make_async_remote_copy(
            src_ref=src, dst_ref=dst, send_sem=send, recv_sem=recv,
            device_id=target, device_id_type=MESH,
        )

    def lanes(h):
        return pl.ds(pl.multiple_of(h * HD, HD), HD)

    small = (
        pltpu.make_async_copy(prof_hbm, prof_ref, loc_sem.at[3]),
        pltpu.make_async_copy(win_hbm, win_ref, loc_sem.at[4]),
    )
    for copy in small:
        copy.start()
    sources = (k_ref, v_ref, q_ref)
    for n, src in enumerate(sources):
        def local_start(h, _):
            pltpu.make_async_copy(src.at[0, :, lanes(h)], full.at[n, h], loc_sem.at[n]).start()
            return 0

        lax.fori_loop(0, here, local_start, 0)

    barrier = pltpu.get_barrier_semaphore()
    for other in others_c:
        pl.semaphore_signal(barrier, inc=1, device_id={"head": other}, device_id_type=MESH)
    for other in others_x:
        pl.semaphore_signal(barrier, inc=1, device_id={"space": other}, device_id_type=MESH)
    for other in others_f:
        pl.semaphore_signal(barrier, inc=1, device_id={"frame": other}, device_id_type=MESH)

    for copy in small:
        copy.wait()

    count = jnp.int32(0)
    for h in range(here):
        count = count + prof_ref[h]
    first_space = (count >= share).astype(jnp.int32)
    main_count = jnp.maximum(count, here - count)
    for e in range(cores):
        main = first_space if e == 0 else 1 - first_space
        major = jnp.int32(0)
        minor = main_count
        for h in range(here):
            p = prof_ref[e * here + h]
            is_main = p * main + (1 - p) * (1 - main)
            slot = jnp.clip(is_main * major + (1 - is_main) * minor, 0, here - 1)
            major = major + is_main
            minor = minor + (1 - is_main)
            away = ((slot >= share) & (slot < main_count)).astype(jnp.int32)
            owner = away * (1 - e) + (1 - away) * e
            pos[e * here + h] = slot
            place[e * here + h] = owner * here + (1 - p) * share + slot - (slot >= share).astype(jnp.int32) * share

    def fill(slot, _):
        for e in range(cores):
            head = jnp.int32(0)
            reach = jnp.int32(0)
            for h in range(here):
                hit = pos[e * here + h] == slot
                head = head + jnp.where(hit, h, 0)
                reach = reach + jnp.where(hit, win_ref[e * here + h], 0)
            order[e, slot] = jnp.clip(head, 0, here - 1)
            reaches[e, slot] = reach
        return 0

    lax.fori_loop(0, here, fill, 0)

    for n in range(3):
        pltpu.make_async_copy(full.at[n], full.at[n], loc_sem.at[n]).wait()

    def arrange(slot, _):
        head = order[c, slot]
        for n in range(3):
            mine_first[slot, n] = full[n, head]
        return 0

    lax.fori_loop(0, here, arrange, 0)

    pl.semaphore_wait(barrier, len(others_c) + len(others_x) + len(others_f))

    partner = others_c[0]

    def core_copy(j):
        return remote(mine_first.at[share + j], theirs.at[j], d_send.at[j], d_recv.at[j], head=partner)

    def core_start(j, _):
        core_copy(j).start()
        return 0

    lax.fori_loop(0, share, core_start, 0)

    main_space = c * (1 - first_space) + (1 - c) * first_space
    my_rows = pl.ds(pl.multiple_of(x * rows, rows), rows)
    mine = pl.ds(pl.multiple_of(f * part, part), part)

    def window_copy(j, other):
        return remote(
            tsend.at[j, other], trecv.at[f, j], t_send.at[other, j], t_recv.at[f, j], frame=other
        )

    def space_copy(j, other):
        return remote(
            kv.at[j, :, my_rows], kv.at[j, :, my_rows], s_send.at[other, j], s_recv.at[x, j], space=other
        )

    def gather(j, _):
        core_copy(j).wait_recv()
        borrowed = share + j < main_count
        for n in range(3):
            head_main = mine_first[j, n]
            head_rest = jnp.where(borrowed, theirs[j, n], mine_first[share + j, n])
            block = jnp.where(main_space == 1, head_rest, head_main)
            for g in range(frames):
                tsend[j, g, n] = block[g * part:(g + 1) * part]
            block = jnp.where(main_space == 1, head_main, head_rest)
            if n < 2:
                kv[j, n, my_rows] = block
            else:
                squery[j] = block
        own_reach = reaches[c, j + main_space * share]
        far_reach = reaches[partner, share + j]
        tab[j] = jnp.where((main_space == 1) & borrowed, far_reach, own_reach)
        for other in far_first:
            window_copy(j, other).start()

        @pl.when(j > 0)
        def _():
            for other in others_x:
                space_copy(j - 1, other).start()

        return 0

    lax.fori_loop(0, share, gather, 0)

    def out_copy(j, other):
        return remote(
            tout.at[j, other], res.at[c * here + share + j, mine], o_send.at[other, j], o_recv.at[f, j], frame=other
        )

    def back_copy(slot, other):
        return remote(
            res.at[c * here + slot], res.at[c * here + slot], r_send.at[other, slot], r_recv.at[c, slot], head=other
        )

    for other in others_x:
        space_copy(share - 1, other).start()

    def step(j, _):
        for other in others_f:
            remote(
                tsend.at[j, other], trecv.at[other, j], t_send.at[other, j], t_recv.at[other, j], frame=other
            ).wait_recv()
        trecv[f, j] = tsend[j, f]
        reach = tab[j]
        qs = [trecv[g, j, 2].astype(jnp.float32) for g in range(frames)]
        ks = [trecv[g, j, 0].astype(jnp.float32) for g in range(frames)]
        vs = [trecv[g, j, 1].astype(jnp.float32) for g in range(frames)]
        for g in range(frames):
            near = [m for m in range(frames) if abs(m - g) <= WMAX]
            scores = []
            for m in near:
                raw = jnp.sum(qs[g] * ks[m], axis=-1, keepdims=True) * scale
                scores.append(jnp.where(reach >= abs(m - g), raw, -1e30))
            peak = functools.reduce(jnp.maximum, scores)
            weights = [jnp.exp(s - peak) for s in scores]
            total = functools.reduce(jnp.add, weights)
            acc = functools.reduce(
                jnp.add,
                [w.astype(jnp.bfloat16).astype(jnp.float32) * vs[m] for w, m in zip(weights, near)],
            )
            tout[j, g] = (acc / total).astype(jnp.bfloat16)
        res[c * here + share + j, mine] = tout[j, f]

        for other in others_x:
            other_rows = pl.ds(pl.multiple_of(other * rows, rows), rows)
            remote(
                kv.at[j, :, other_rows], kv.at[j, :, other_rows],
                s_send.at[other, j], s_recv.at[other, j], space=other,
            ).wait_recv()
        query = squery[j]
        scores = lax.dot_general(
            query, kv[j, 0], (((1,), (1,)), ((), ())), preferred_element_type=jnp.float32
        ) * scale
        peak = jnp.max(scores, axis=1, keepdims=True)
        weights = jnp.exp(scores - peak)
        total = jnp.sum(weights, axis=1, keepdims=True)
        acc = jnp.dot(weights.astype(jnp.bfloat16), kv[j, 1], preferred_element_type=jnp.float32)
        res[c * here + j] = (acc / total).astype(jnp.bfloat16)

        for other in far_first:
            out_copy(j, other).start()

        @pl.when(j > 0)
        def _():
            for other in others_c:
                back_copy(j - 1, other).start()

        return 0

    lax.fori_loop(0, share, step, 0)
    for other in others_c:
        back_copy(share - 1, other).start()

    def forward(j, _):
        for other in others_f:
            theirs = pl.ds(pl.multiple_of(other * part, part), part)
            remote(
                tout.at[j, other], res.at[c * here + share + j, theirs], o_send.at[other, j], o_recv.at[other, j],
                frame=other,
            ).wait_recv()
        for other in others_c:
            back_copy(share + j, other).start()
        return 0

    lax.fori_loop(0, share, forward, 0)

    def arrive(slot, _):
        for other in others_c:
            remote(
                res.at[c * here + slot], res.at[other * here + slot], r_send.at[other, slot], r_recv.at[other, slot], head=other
            ).wait_recv()
        return 0

    lax.fori_loop(0, 2 * share, arrive, 0)

    for i in range(here):
        out_ref[0, :, i * HD:(i + 1) * HD] = res[place[c * here + i]]


    def drain(j, _):
        core_copy(j).wait_send()
        for other in others_f:
            window_copy(j, other).wait_send()
            out_copy(j, other).wait_send()
        for other in others_x:
            space_copy(j, other).wait_send()
        for other in others_c:
            back_copy(j, other).wait_send()
            back_copy(share + j, other).wait_send()
        return 0

    lax.fori_loop(0, share, drain, 0)


def local(sizes, queries, key_states, value_states, profile, window):
    frames, spaces, cores = sizes
    rows = queries.shape[1]
    here = queries.shape[2] // HD
    share = here // 2
    part = rows // frames
    any_space = pl.BlockSpec(memory_space=pl.ANY)
    bf = jnp.bfloat16
    dma = pltpu.SemaphoreType.DMA
    return pl.pallas_call(
        functools.partial(kernel, frames, spaces, cores),
        out_shape=pltpu.VMEM(queries.shape, queries.dtype),
        in_specs=[any_space] * 5,
        out_specs=pl.BlockSpec(memory_space=pltpu.VMEM),
        scratch_shapes=[
            pltpu.VMEM((3, here, rows, HD), bf),
            pltpu.VMEM((here, 3, rows, HD), bf),
            pltpu.VMEM((share, 3, rows, HD), bf),
            pltpu.VMEM((share, rows, HD), bf),
            pltpu.VMEM((share, 2, spaces * rows, HD), bf),
            pltpu.VMEM((share, frames, 3, part, HD), bf),
            pltpu.VMEM((frames, share, 3, part, HD), bf),
            pltpu.VMEM((share, frames, part, HD), bf),
            pltpu.VMEM((cores * 2 * share, rows, HD), bf),
            pltpu.SMEM((here * cores,), jnp.int32),
            pltpu.SMEM((here * cores,), jnp.int32),
            pltpu.SMEM((here * cores,), jnp.int32),
            pltpu.SMEM((here * cores,), jnp.int32),
            pltpu.SMEM((cores, here), jnp.int32),
            pltpu.SMEM((cores, here), jnp.int32),
            pltpu.SMEM((share,), jnp.int32),
            dma((5,)),
            dma((share,)),
            dma((share,)),
            dma((spaces, share)),
            dma((spaces, share)),
            dma((frames, share)),
            dma((frames, share)),
            dma((frames, share)),
            dma((frames, share)),
            dma((cores, 2 * share)),
            dma((cores, 2 * share)),
        ],
        compiler_params=pltpu.CompilerParams(
            collective_id=0, has_side_effects=True, vmem_limit_bytes=60 * 1024 * 1024
        ),
    )(profile, window, queries, key_states, value_states)


def solution(mesh):
    spec = P(("groups", "frame"), "space", "head")
    sizes = (mesh.shape["frame"], mesh.shape["space"], mesh.shape["head"])
    return jax.shard_map(
        functools.partial(local, sizes),
        mesh=mesh,
        in_specs=(spec, spec, spec, P(), P()),
        out_specs=spec,
        check_vma=False,
    )
```

```python
import functools

import jax
import jax.numpy as jnp
from jax import lax
from jax.experimental import pallas as pl
from jax.experimental.pallas import tpu as pltpu
from jax.sharding import PartitionSpec as P

HD = 128
WMAX = 4
MESH = pl.DeviceIdType.MESH


def kernel(
    frames, spaces, cores, prof_hbm, win_hbm, q_ref, k_ref, v_ref, out_ref,
    full, mine_first, theirs, squery, kv, tsend, trecv, tout, res,
    prof_ref, win_ref, pos, place, order, tab,
    loc_sem, d_send, d_recv, s_send, s_recv, t_send, t_recv, o_send, o_recv, r_send, r_recv,
):
    rows = q_ref.shape[1]
    here = q_ref.shape[2] // HD
    share = here // 2
    part = rows // frames
    scale = HD ** (-0.5)
    f = lax.axis_index("frame")
    x = lax.axis_index("space")
    c = lax.axis_index("head")
    others_f = [lax.rem(f + d, frames) for d in range(1, frames)]
    others_x = [lax.rem(x + d, spaces) for d in range(1, spaces)]
    others_c = [lax.rem(c + d, cores) for d in range(1, cores)]
    side = f // (frames // 2)
    far_first = [
        lax.rem(f + (1 - side) * (frames - 1 - i) + side * (1 + i), frames)
        for i in range(frames - 1)
    ]

    def remote(src, dst, send, recv, **target):
        return pltpu.make_async_remote_copy(
            src_ref=src, dst_ref=dst, send_sem=send, recv_sem=recv,
            device_id=target, device_id_type=MESH,
        )

    def lanes(h):
        return pl.ds(pl.multiple_of(h * HD, HD), HD)

    small = (
        pltpu.make_async_copy(prof_hbm, prof_ref, loc_sem.at[3]),
        pltpu.make_async_copy(win_hbm, win_ref, loc_sem.at[4]),
    )
    for copy in small:
        copy.start()
    sources = (k_ref, v_ref, q_ref)
    for n, src in enumerate(sources):
        def local_start(h, _):
            pltpu.make_async_copy(src.at[0, :, lanes(h)], full.at[n, h], loc_sem.at[n]).start()
            return 0

        lax.fori_loop(0, here, local_start, 0)

    barrier = pltpu.get_barrier_semaphore()
    for other in others_c:
        pl.semaphore_signal(barrier, inc=1, device_id={"head": other}, device_id_type=MESH)
    for other in others_x:
        pl.semaphore_signal(barrier, inc=1, device_id={"space": other}, device_id_type=MESH)
    for other in others_f:
        pl.semaphore_signal(barrier, inc=1, device_id={"frame": other}, device_id_type=MESH)

    for copy in small:
        copy.wait()

    count = jnp.int32(0)
    for h in range(here):
        count = count + prof_ref[h]
    first_space = (count >= share).astype(jnp.int32)
    main_count = jnp.maximum(count, here - count)
    for e in range(cores):
        main = first_space if e == 0 else 1 - first_space
        major = jnp.int32(0)
        minor = main_count
        for h in range(here):
            p = prof_ref[e * here + h]
            is_main = p * main + (1 - p) * (1 - main)
            slot = jnp.clip(is_main * major + (1 - is_main) * minor, 0, here - 1)
            major = major + is_main
            minor = minor + (1 - is_main)
            away = ((slot >= share) & (slot < main_count)).astype(jnp.int32)
            owner = away * (1 - e) + (1 - away) * e
            pos[e * here + h] = slot
            place[e * here + h] = owner * here + (1 - p) * share + slot - (slot >= share).astype(jnp.int32) * share

    def fill(slot, _):
        head = jnp.int32(0)
        for h in range(here):
            head = head + jnp.where(pos[c * here + h] == slot, h, 0)
        order[slot] = jnp.clip(head, 0, here - 1)
        return 0

    lax.fori_loop(0, here, fill, 0)

    for n in range(3):
        pltpu.make_async_copy(full.at[n], full.at[n], loc_sem.at[n]).wait()

    def arrange(slot, _):
        head = order[slot]
        for n in range(3):
            mine_first[slot, n] = full[n, head]
        return 0

    lax.fori_loop(0, here, arrange, 0)

    pl.semaphore_wait(barrier, len(others_c) + len(others_x) + len(others_f))

    partner = others_c[0]

    def core_copy(j):
        return remote(mine_first.at[share + j], theirs.at[j], d_send.at[j], d_recv.at[j], head=partner)

    def core_start(j, _):
        core_copy(j).start()
        return 0

    lax.fori_loop(0, share, core_start, 0)

    main_space = c * (1 - first_space) + (1 - c) * first_space
    my_rows = pl.ds(pl.multiple_of(x * rows, rows), rows)
    mine = pl.ds(pl.multiple_of(f * part, part), part)

    def window_copy(j, other):
        return remote(
            tsend.at[j, other], trecv.at[f, j], t_send.at[other, j], t_recv.at[f, j], frame=other
        )

    def space_copy(j, other):
        return remote(
            kv.at[j, :, my_rows], kv.at[j, :, my_rows], s_send.at[other, j], s_recv.at[x, j], space=other
        )

    def gather(j, _):
        core_copy(j).wait_recv()
        borrowed = share + j < main_count
        for n in range(3):
            head_main = mine_first[j, n]
            head_rest = jnp.where(borrowed, theirs[j, n], mine_first[share + j, n])
            block = jnp.where(main_space == 1, head_rest, head_main)
            for g in range(frames):
                tsend[j, g, n] = block[g * part:(g + 1) * part]
            block = jnp.where(main_space == 1, head_main, head_rest)
            if n < 2:
                kv[j, n, my_rows] = block
            else:
                squery[j] = block
        for other in far_first:
            window_copy(j, other).start()

        @pl.when(j > 0)
        def _():
            for other in others_x:
                space_copy(j - 1, other).start()

        return 0

    lax.fori_loop(0, share, gather, 0)

    def fill_reach(j, _):
        own_slot = j + main_space * share
        far = ((main_space == 1) & (share + j < main_count)).astype(jnp.int32)
        own_reach = jnp.int32(0)
        far_reach = jnp.int32(0)
        for h in range(here):
            own_reach = own_reach + jnp.where(pos[c * here + h] == own_slot, win_ref[c * here + h], 0)
            far_reach = far_reach + jnp.where(
                pos[partner * here + h] == share + j, win_ref[partner * here + h], 0
            )
        tab[j] = far * far_reach + (1 - far) * own_reach
        return 0

    lax.fori_loop(0, share, fill_reach, 0)

    def out_copy(j, other):
        return remote(
            tout.at[j, other], res.at[c * here + share + j, mine], o_send.at[other, j], o_recv.at[f, j], frame=other
        )

    def back_copy(slot, other):
        return remote(
            res.at[c * here + slot], res.at[c * here + slot], r_send.at[other, slot], r_recv.at[c, slot], head=other
        )

    for other in others_x:
        space_copy(share - 1, other).start()

    def step(j, _):
        for other in others_f:
            remote(
                tsend.at[j, other], trecv.at[other, j], t_send.at[other, j], t_recv.at[other, j], frame=other
            ).wait_recv()
        trecv[f, j] = tsend[j, f]
        reach = tab[j]
        qs = [trecv[g, j, 2].astype(jnp.float32) for g in range(frames)]
        ks = [trecv[g, j, 0].astype(jnp.float32) for g in range(frames)]
        vs = [trecv[g, j, 1].astype(jnp.float32) for g in range(frames)]
        for g in range(frames):
            near = [m for m in range(frames) if abs(m - g) <= WMAX]
            scores = []
            for m in near:
                raw = jnp.sum(qs[g] * ks[m], axis=-1, keepdims=True) * scale
                scores.append(jnp.where(reach >= abs(m - g), raw, -1e30))
            peak = functools.reduce(jnp.maximum, scores)
            weights = [jnp.exp(s - peak) for s in scores]
            total = functools.reduce(jnp.add, weights)
            acc = functools.reduce(
                jnp.add,
                [w.astype(jnp.bfloat16).astype(jnp.float32) * vs[m] for w, m in zip(weights, near)],
            )
            tout[j, g] = (acc / total).astype(jnp.bfloat16)
        res[c * here + share + j, mine] = tout[j, f]

        for other in others_x:
            other_rows = pl.ds(pl.multiple_of(other * rows, rows), rows)
            remote(
                kv.at[j, :, other_rows], kv.at[j, :, other_rows],
                s_send.at[other, j], s_recv.at[other, j], space=other,
            ).wait_recv()
        query = squery[j]
        scores = lax.dot_general(
            query, kv[j, 0], (((1,), (1,)), ((), ())), preferred_element_type=jnp.float32
        ) * scale
        peak = jnp.max(scores, axis=1, keepdims=True)
        weights = jnp.exp(scores - peak)
        total = jnp.sum(weights, axis=1, keepdims=True)
        acc = jnp.dot(weights.astype(jnp.bfloat16), kv[j, 1], preferred_element_type=jnp.float32)
        res[c * here + j] = (acc / total).astype(jnp.bfloat16)

        for other in far_first:
            out_copy(j, other).start()

        @pl.when(j > 0)
        def _():
            for other in others_c:
                back_copy(j - 1, other).start()

        return 0

    lax.fori_loop(0, share, step, 0)
    for other in others_c:
        back_copy(share - 1, other).start()

    def forward(j, _):
        for other in others_f:
            theirs = pl.ds(pl.multiple_of(other * part, part), part)
            remote(
                tout.at[j, other], res.at[c * here + share + j, theirs], o_send.at[other, j], o_recv.at[other, j],
                frame=other,
            ).wait_recv()
        for other in others_c:
            back_copy(share + j, other).start()
        return 0

    lax.fori_loop(0, share, forward, 0)

    def arrive(slot, _):
        for other in others_c:
            remote(
                res.at[c * here + slot], res.at[other * here + slot], r_send.at[other, slot], r_recv.at[other, slot], head=other
            ).wait_recv()
        return 0

    lax.fori_loop(0, 2 * share, arrive, 0)

    for i in range(here):
        out_ref[0, :, i * HD:(i + 1) * HD] = res[place[c * here + i]]


    def drain(j, _):
        core_copy(j).wait_send()
        for other in others_f:
            window_copy(j, other).wait_send()
            out_copy(j, other).wait_send()
        for other in others_x:
            space_copy(j, other).wait_send()
        for other in others_c:
            back_copy(j, other).wait_send()
            back_copy(share + j, other).wait_send()
        return 0

    lax.fori_loop(0, share, drain, 0)


def local(sizes, queries, key_states, value_states, profile, window):
    frames, spaces, cores = sizes
    rows = queries.shape[1]
    here = queries.shape[2] // HD
    share = here // 2
    part = rows // frames
    any_space = pl.BlockSpec(memory_space=pl.ANY)
    bf = jnp.bfloat16
    dma = pltpu.SemaphoreType.DMA
    return pl.pallas_call(
        functools.partial(kernel, frames, spaces, cores),
        out_shape=pltpu.VMEM(queries.shape, queries.dtype),
        in_specs=[any_space] * 5,
        out_specs=pl.BlockSpec(memory_space=pltpu.VMEM),
        scratch_shapes=[
            pltpu.VMEM((3, here, rows, HD), bf),
            pltpu.VMEM((here, 3, rows, HD), bf),
            pltpu.VMEM((share, 3, rows, HD), bf),
            pltpu.VMEM((share, rows, HD), bf),
            pltpu.VMEM((share, 2, spaces * rows, HD), bf),
            pltpu.VMEM((share, frames, 3, part, HD), bf),
            pltpu.VMEM((frames, share, 3, part, HD), bf),
            pltpu.VMEM((share, frames, part, HD), bf),
            pltpu.VMEM((cores * 2 * share, rows, HD), bf),
            pltpu.SMEM((here * cores,), jnp.int32),
            pltpu.SMEM((here * cores,), jnp.int32),
            pltpu.SMEM((here * cores,), jnp.int32),
            pltpu.SMEM((here * cores,), jnp.int32),
            pltpu.SMEM((here,), jnp.int32),
            pltpu.SMEM((share,), jnp.int32),
            dma((5,)),
            dma((share,)),
            dma((share,)),
            dma((spaces, share)),
            dma((spaces, share)),
            dma((frames, share)),
            dma((frames, share)),
            dma((frames, share)),
            dma((frames, share)),
            dma((cores, 2 * share)),
            dma((cores, 2 * share)),
        ],
        compiler_params=pltpu.CompilerParams(
            collective_id=0, has_side_effects=True, vmem_limit_bytes=60 * 1024 * 1024
        ),
    )(profile, window, queries, key_states, value_states)


def solution(mesh):
    spec = P(("groups", "frame"), "space", "head")
    sizes = (mesh.shape["frame"], mesh.shape["space"], mesh.shape["head"])
    return jax.shard_map(
        functools.partial(local, sizes),
        mesh=mesh,
        in_specs=(spec, spec, spec, P(), P()),
        out_specs=spec,
        check_vma=False,
    )
```
